32 devices in a mesh: task: 4 (over x, core), dp: 8 (over z, y).
Axes of the slice: x: 2, y: 2, z: 4, core: 2. Of those that a mesh axis runs over, the one named last changes fastest.
Arguments:
- inputs: bfloat16 [4, 2, 4096, 1024], P('task', None, 'dp'), may hold values from -48 to 48
- labels: int32 [4, 2, 4096], P('task', None, 'dp'), may hold values from 0 to 999
- w_hidden: float32 [4, 1024, 1024], P('task', 'dp'), may hold values from -6 to 6
- w_out: float32 [4, 1024, 1000], P('task', 'dp'), may hold values from -12 to 12
- mom_hidden: float32 [4, 1024, 1024], P('task', 'dp'), may hold values from -0.6 to 0.6
- mom_out: float32 [4, 1024, 1000], P('task', 'dp'), may hold values from -0.6 to 0.6
- signs: int32 [4], P('task'), may hold values from -1 to 1, as said below
- perturb: float32 [4, 512, 512], P('task', 'dp'), may hold values from -6 to 6
- hyper_in: float32 [8, 512], replicated, may hold values from -2 to 2
- hyper_mid: float32 [512, 512], P('dp'), may hold values from -0.25 to 0.25
- hyper_out: float32 [512, 21], replicated, may hold values from -0.25 to 0.25
Outputs:
- new_hidden: float32 [4, 1024, 1024], P('task', 'dp')
- new_out: float32 [4, 1024, 1000], P('task', 'dp')
- new_mom_hidden: float32 [4, 1024, 1024], P('task', 'dp')
- new_mom_out: float32 [4, 1024, 1000], P('task', 'dp')
- task_losses: float32 [4, 2], P('task')
- meta_grad: float32 [512, 512], P('dp')
The draws below stay inside these ranges and needn't reach their ends.
Inputs may be any that keep to these rules, and one draw needn't show every extreme that they name: `signs`: each entry is +1 or -1.
All inputs are finite; a program needn't handle non-finite values.
Results may differ from the reference program's by a relative error of at most 0.01045.
The reference program's roundings to bfloat16 on the way count: a program that leaves them out, or rounds other values in their place, can miss the bound.
Values may be sent and summed in bfloat16 or wider, within the bound.
A program may use at most 128 MiB of HBM per device.

```python
import jax
import jax.numpy as jnp
from jax import lax

DIN = 1024
HID = 1024
CLASSES = 1000
HYP = 512
TFEAT = 8
STEPS = 2
NGEN = 21
BATCH = 4096
TASKS = 4


def draw_inputs(key, part):
    base_key = jax.random.fold_in(key, 0)
    values = jnp.clip(jax.random.normal(base_key, (TASKS, STEPS, BATCH, DIN), jnp.float32), -6.0, 6.0)
    return values.astype(jnp.bfloat16)


def draw_w_out(key, part):
    base_key = jax.random.fold_in(key, 0)
    values = jnp.clip(jax.random.normal(base_key, (TASKS, HID, CLASSES), jnp.float32), -6.0, 6.0)
    return values


def draw_signs(key, part):
    return (2 * jax.random.randint(key, (TASKS,), 0, 2) - 1).astype(jnp.int32)


def with_ends(entries, own_key, low, top_value):
    extent = entries.shape
    spot = [jax.random.randint(jax.random.fold_in(own_key, axis), (), 0, extent[axis]) for axis in range(len(extent))]
    entries = entries.at[tuple(spot)].set(low)
    longest = extent.index(max(extent))
    spot[longest] = (spot[longest] + 1) % extent[longest]
    return entries.at[tuple(spot)].set(top_value)


def shard_levels(stream_key, dims, pieces, least, largest):
    level, own = 1.0, jax.random.fold_in(stream_key, 6)
    for dim, shards_of in pieces:
        heights = jnp.exp(jax.random.uniform(jax.random.fold_in(own, dim), (shards_of,), jnp.float32, least / len(pieces), largest / len(pieces)))
        level = level * jnp.repeat(heights, dims[dim] // shards_of).reshape([-1 if axis == dim else 1 for axis in range(len(dims))])
    return level


def gaussian(key, extent, deviation, bound, pieces=(), kind=jnp.bfloat16):
    array = deviation * jax.random.normal(key, extent, jnp.float32)
    if pieces:
        array = array * shard_levels(key, extent, pieces, -0.22, 0.18)
    return jnp.clip(array, -bound, bound).astype(kind)


def setup_inputs(seed: int = 0) -> dict:
    keys = jax.random.split(jax.random.key(seed), 12)
    inputs = draw_inputs(jax.random.fold_in(keys[11], 71), 0)
    labels = with_ends(jax.random.randint(keys[1], (TASKS, STEPS, BATCH), 0, CLASSES), jax.random.fold_in(keys[1], 1), 0, CLASSES - 1).astype(jnp.int32)
    w_hidden = gaussian(keys[2], (TASKS, DIN, HID), 1.0, 6.0, ((0, 4), (1, 8)), jnp.float32)
    w_out = draw_w_out(jax.random.fold_in(keys[11], 71), 0)
    mom_hidden = gaussian(keys[4], (TASKS, DIN, HID), 0.1, 0.6, ((0, 4), (1, 8)), jnp.float32)
    mom_out = gaussian(keys[5], (TASKS, HID, CLASSES), 0.1, 0.6, ((0, 4), (1, 8)), jnp.float32)
    signs = draw_signs(jax.random.fold_in(keys[11], 71), 0)
    perturb = gaussian(keys[7], (TASKS, HYP, HYP), 1.0, 6.0, ((0, 4), (1, 8)), jnp.float32)
    hyper_in = gaussian(keys[8], (TFEAT, HYP), TFEAT ** -0.5, 2.0, (), jnp.float32)
    hyper_mid = gaussian(keys[9], (HYP, HYP), HYP ** -0.5, 0.25, ((0, 8),), jnp.float32)
    hyper_out = gaussian(keys[10], (HYP, NGEN), HYP ** -0.5, 0.25, (), jnp.float32)
    return dict(inputs=inputs, labels=labels, w_hidden=w_hidden, w_out=w_out, mom_hidden=mom_hidden, mom_out=mom_out, signs=signs, perturb=perturb, hyper_in=hyper_in, hyper_mid=hyper_mid, hyper_out=hyper_out)


BETA = 0.8
FLOOR = 0.001
SIGMA = 0.01
LR_BASE = 0.03
HIGH = lax.Precision.HIGHEST

def moment_sums(gradient, moment, tensor):
    return jnp.stack([jnp.sum(gradient * gradient), jnp.sum(moment * moment), jnp.sum(tensor * tensor), jnp.sum(gradient * moment)])

def tensor_inputs(sums, step, steps):
    grad_sq = sums[:, 0]
    moment_sq = sums[:, 1]
    weight_sq = sums[:, 2]
    cross_term = sums[:, 3]
    kind_table = jnp.eye(2, dtype=jnp.float32)
    step_share = jnp.full((2,), (step + 1.0) / steps, jnp.float32)
    return jnp.stack([jnp.log(FLOOR + grad_sq), jnp.log(FLOOR + moment_sq), jnp.log(1.0 + weight_sq), cross_term / jnp.sqrt((FLOOR + grad_sq) * (FLOOR + moment_sq)), step_share, jnp.ones((2,), jnp.float32), kind_table[:, 0], kind_table[:, 1]], axis=1)

def apply_rule(tensor, gradient, moment, sums_row, coeffs):
    neurons = (coeffs.shape[0] - 1) // 5
    feat_grad = gradient / jnp.sqrt(FLOOR + sums_row[0])
    feat_moment = moment / jnp.sqrt(FLOOR + sums_row[1])
    direction = jnp.zeros_like(tensor)
    for neuron in range(neurons):
        inner = coeffs[3 * neuron] * feat_grad + coeffs[3 * neuron + 1] * feat_moment + coeffs[3 * neuron + 2] * tensor + coeffs[3 * neurons + neuron]
        direction = direction + coeffs[4 * neurons + neuron] * jnp.maximum(inner, 0.0)
    return tensor - LR_BASE * jnp.exp(coeffs[5 * neurons]) * direction

def reference(inputs, labels, w_hidden, w_out, mom_hidden, mom_out, signs, perturb, hyper_in, hyper_mid, hyper_out):

    def run_task(operands):
        features, classes, hidden_w, out_w, hidden_m, out_m, sign, noise = operands
        theta = hyper_mid + SIGMA * sign.astype(jnp.float32) * noise
        losses = []
        for step in range(STEPS):
            batch_in = features[step]
            hidden_b = hidden_w.astype(jnp.bfloat16)
            out_b = out_w.astype(jnp.bfloat16)
            before = jnp.dot(batch_in, hidden_b, preferred_element_type=jnp.float32) * DIN ** (-0.5)
            active = jnp.maximum(before, 0.0).astype(jnp.bfloat16)
            logits = jnp.dot(active, out_b, preferred_element_type=jnp.float32) * HID ** (-0.5)
            shifted = logits - lax.optimization_barrier(jnp.max(logits, axis=1, keepdims=True))
            log_total = jnp.log(lax.optimization_barrier(jnp.sum(jnp.exp(shifted), axis=1, keepdims=True)))
            onehot = (classes[step][:, None] == jnp.arange(CLASSES, dtype=jnp.int32)[None, :]).astype(jnp.float32)
            example_loss = log_total[:, 0] - lax.optimization_barrier(jnp.sum(shifted * onehot, axis=1))
            losses.append(jnp.sum(example_loss) / BATCH)
            errors = (jnp.exp(shifted - log_total) - onehot).astype(jnp.bfloat16)
            grad_out = jnp.dot(active.T, errors, preferred_element_type=jnp.float32) * HID ** (-0.5)
            back = jnp.dot(errors, out_b.T, preferred_element_type=jnp.float32) * HID ** (-0.5)
            back_pre = jnp.where(before > 0, back, 0.0).astype(jnp.bfloat16)
            grad_hidden = jnp.dot(batch_in.T, back_pre, preferred_element_type=jnp.float32) * DIN ** (-0.5)
            hidden_m = BETA * hidden_m + (1.0 - BETA) * grad_hidden
            out_m = BETA * out_m + (1.0 - BETA) * grad_out
            sums = jnp.stack([moment_sums(grad_hidden, hidden_m, hidden_w) / (DIN * HID), moment_sums(grad_out, out_m, out_w) / (HID * CLASSES)])
            opening = jnp.tanh(jnp.dot(tensor_inputs(sums, step, STEPS), hyper_in, precision=HIGH))
            middle = jnp.tanh(jnp.dot(opening, theta, precision=HIGH))
            coeffs = jnp.dot(middle, hyper_out, precision=HIGH)
            hidden_w = apply_rule(hidden_w, grad_hidden, hidden_m, sums[0], coeffs[0])
            out_w = apply_rule(out_w, grad_out, out_m, sums[1], coeffs[1])
        return (hidden_w, out_w, hidden_m, out_m, jnp.stack(losses))
    new_hidden, new_out, new_mh, new_mo, task_losses = lax.map(run_task, (inputs, labels, w_hidden, w_out, mom_hidden, mom_out, signs, perturb))
    score = lax.optimization_barrier(jnp.sum(task_losses, axis=1)) / STEPS
    center = jnp.sum(score) / TASKS
    weights = signs.astype(jnp.float32) * (score - center) / (SIGMA * TASKS)
    meta_grad = jnp.tensordot(weights, perturb, axes=1, precision=HIGH)
    return (new_hidden, new_out, new_mh, new_mo, task_losses, meta_grad)
```

```python
import functools

import jax
import jax.numpy as jnp
from jax import lax
from jax.experimental import pallas as pl
from jax.experimental.pallas import tpu as pltpu
from jax.sharding import PartitionSpec as P

BETA = 0.8
FLOOR = 0.001
SIGMA = 0.01
LR_BASE = 0.03
LANES = 128
HIGH = lax.Precision.HIGHEST
BY_ROWS = (((0,), (0,)), ((), ()))
BY_COLUMNS = (((1,), (1,)), ((), ()))
MESH = pl.DeviceIdType.MESH
F32 = jnp.float32
BF16 = jnp.bfloat16

HIDDEN_W, OUT_W, OUT_G, HIDDEN_G, STATS, SHARE = range(6)
NOISE, SCORE = range(2)


def fold(value):
    rows, columns = value.shape
    total = value[0:8]
    for row in range(8, rows, 8):
        total = total + value[row : row + 8]
    out = total[:, 0:LANES]
    for column in range(LANES, columns, LANES):
        out = out + total[:, column : column + LANES]
    return out


def full_sum(value):
    return jnp.sum(jnp.sum(value, axis=1, keepdims=True), axis=0, keepdims=True)


def kernel(
    n,
    tasks,
    x_ref,
    label_ref,
    w1_ref,
    w2_ref,
    m1_ref,
    m2_ref,
    sign_ref,
    noise_ref,
    hin_ref,
    mid_ref,
    hout_ref,
    p1,
    new_out,
    q1,
    new_mom_out,
    loss_ref,
    meta_ref,
    full1,
    full2,
    send1,
    send2,
    recv1,
    recv2,
    act,
    err,
    dpre,
    p2,
    q2,
    g1,
    g2,
    example,
    stat_send,
    stat_recv,
    share_send,
    share_recv,
    hout,
    losses,
    noise_send,
    noise_recv,
    score_send,
    score_recv,
    send_sem,
    recv_sem,
    task_send_sem,
    task_recv_sem,
):
    me = lax.axis_index("dp")
    task = lax.axis_index("task")
    steps, local_batch, width_in = x_ref.shape
    rows1 = w1_ref.shape[0]
    rows2, class_count = w2_ref.shape
    width_hidden = w1_ref.shape[1]
    padded = p2.shape[1]
    hyper_rows = mid_ref.shape[0]
    chunk = min(256, local_batch)
    block = min(256, width_hidden, width_in)
    scale_in = width_in ** (-0.5)
    scale_hidden = width_hidden ** (-0.5)
    batch_total = local_batch * n
    lane8 = lax.broadcasted_iota(jnp.int32, (8, LANES), 1)
    row8 = lax.broadcasted_iota(jnp.int32, (8, LANES), 0)

    barrier = pltpu.get_barrier_semaphore()

    @pl.loop(1, n)
    def _(k):
        pl.semaphore_signal(
            barrier, inc=1, device_id={"dp": lax.rem(me + k, n)}, device_id_type=MESH
        )

    @pl.loop(1, tasks)
    def _(k):
        pl.semaphore_signal(
            barrier, inc=1, device_id={"task": lax.rem(task + k, tasks)}, device_id_type=MESH
        )

    p1[...] = w1_ref[...]
    q1[...] = m1_ref[...]
    p2[...] = jnp.zeros_like(p2)
    q2[...] = jnp.zeros_like(q2)
    p2[:, 0:class_count] = w2_ref[...]
    q2[:, 0:class_count] = m2_ref[...]
    hout[...] = jnp.zeros_like(hout)
    hout[:, 0 : hout_ref.shape[1]] = hout_ref[...]
    noise_send[...] = noise_ref[...]
    pl.semaphore_wait(barrier, n - 1 + tasks - 1)

    def noise_copy(k):
        return pltpu.make_async_remote_copy(
            src_ref=noise_send,
            dst_ref=noise_recv.at[k],
            send_sem=task_send_sem.at[NOISE, k],
            recv_sem=task_recv_sem.at[NOISE, k],
            device_id={"task": lax.rem(task + k, tasks)},
            device_id_type=MESH,
        )

    def score_copy(k):
        return pltpu.make_async_remote_copy(
            src_ref=score_send,
            dst_ref=score_recv.at[k],
            send_sem=task_send_sem.at[SCORE, k],
            recv_sem=task_recv_sem.at[SCORE, k],
            device_id={"task": lax.rem(task + k, tasks)},
            device_id_type=MESH,
        )

    def one_step(step, carry):
        def copy(stage, k):
            peer = lax.rem(me + k, n)
            if stage == HIDDEN_W:
                own = full1.at[step, pl.ds(pl.multiple_of(me * rows1, rows1), rows1)]
                source, target = own, own
            elif stage == OUT_W:
                own = full2.at[step, pl.ds(pl.multiple_of(me * rows2, rows2), rows2)]
                source, target = own, own
            elif stage == OUT_G:
                source = send2.at[step, pl.ds(pl.multiple_of(peer * rows2, rows2), rows2)]
                target = recv2.at[step, k]
            elif stage == HIDDEN_G:
                source = send1.at[step, pl.ds(pl.multiple_of(peer * rows1, rows1), rows1)]
                target = recv1.at[step, k]
            elif stage == STATS:
                source, target = stat_send.at[step], stat_recv.at[step, k]
            else:
                source, target = share_send.at[step], share_recv.at[step, k]
            return pltpu.make_async_remote_copy(
                src_ref=source,
                dst_ref=target,
                send_sem=send_sem.at[step, stage, k],
                recv_sem=recv_sem.at[step, stage, k],
                device_id={"dp": peer},
                device_id_type=MESH,
            )

        def start(stage):
            @pl.loop(1, n)
            def _(k):
                copy(stage, k).start()

        def arrive(stage):
            @pl.loop(1, n)
            def _(k):
                copy(stage, k).wait_recv()

        full1[step, pl.ds(pl.multiple_of(me * rows1, rows1), rows1)] = p1[...].astype(BF16)
        full2[step, pl.ds(pl.multiple_of(me * rows2, rows2), rows2)] = p2[...].astype(BF16)
        start(HIDDEN_W)
        start(OUT_W)

        arrive(HIDDEN_W)

        @pl.loop(0, local_batch // chunk)
        def _(i):
            at = pl.ds(pl.multiple_of(i * chunk, chunk), chunk)
            pre = jnp.dot(x_ref[step, at, :], full1[step], preferred_element_type=F32)
            act[at, :] = jnp.maximum(pre * scale_in, 0.0).astype(BF16)

        arrive(OUT_W)

        @pl.loop(0, local_batch // chunk)
        def _(i):
            at = pl.ds(pl.multiple_of(i * chunk, chunk), chunk)
            logits = jnp.dot(act[at, :], full2[step], preferred_element_type=F32) * scale_hidden
            column = lax.broadcasted_iota(jnp.int32, logits.shape, 1)
            logits = jnp.where(column < class_count, logits, -jnp.inf)
            shifted = logits - jnp.max(logits, axis=1, keepdims=True)
            weight = jnp.exp(shifted)
            total = jnp.sum(weight, axis=1, keepdims=True)
            hit = column == label_ref[step, at, :]
            picked = jnp.sum(jnp.where(hit, shifted, 0.0), axis=1, keepdims=True)
            example[at, :] = jnp.log(total) - picked
            err[at, :] = (weight * (1.0 / total) - jnp.where(hit, 1.0, 0.0)).astype(BF16)

        @pl.loop(0, width_hidden // block)
        def _(i):
            at = pl.ds(pl.multiple_of(i * block, block), block)
            grad = lax.dot_general(act[:, at], err[...], BY_ROWS, preferred_element_type=F32)
            send2[step, at, :] = grad.astype(BF16)

        start(OUT_G)

        @pl.loop(0, local_batch // chunk)
        def _(i):
            at = pl.ds(pl.multiple_of(i * chunk, chunk), chunk)
            back = lax.dot_general(err[at, :], full2[step], BY_COLUMNS, preferred_element_type=F32)
            live = act[at, :].astype(F32) > 0.0
            dpre[at, :] = jnp.where(live, back * scale_hidden, 0.0).astype(BF16)

        @pl.loop(0, width_in // block)
        def _(i):
            at = pl.ds(pl.multiple_of(i * block, block), block)
            grad = lax.dot_general(x_ref[step, :, at], dpre[...], BY_ROWS, preferred_element_type=F32)
            send1[step, at, :] = grad.astype(BF16)

        start(HIDDEN_G)

        def reduce(sent, received, gradient, moment, tensor, rows, scale):
            def body(i, sums):
                offset = pl.multiple_of(i * 16, 16)
                at = pl.ds(offset, 16)
                own = pl.ds(pl.multiple_of(me * rows + offset, 16), 16)
                grad = sent[step, own, :].astype(F32)
                for k in range(1, n):
                    grad = grad + received[step, k, at, :].astype(F32)
                grad = grad * scale
                mom = BETA * moment[at, :] + (1.0 - BETA) * grad
                value = tensor[at, :]
                gradient[at, :] = grad
                moment[at, :] = mom
                return (
                    sums[0] + fold(grad * grad),
                    sums[1] + fold(mom * mom),
                    sums[2] + fold(value * value),
                    sums[3] + fold(grad * mom),
                )

            zero = jnp.zeros((8, LANES), F32)
            return lax.fori_loop(0, rows // 16, body, (zero, zero, zero, zero))

        arrive(OUT_G)
        sums2 = reduce(send2, recv2, g2, q2, p2, rows2, scale_hidden)
        arrive(HIDDEN_G)
        sums1 = reduce(send1, recv1, g1, q1, p1, rows1, scale_in)
        tile = jnp.zeros((8, LANES), F32)
        for row, sums in enumerate((sums1, sums2)):
            for lane, value in enumerate(sums):
                tile = tile + jnp.where((row8 == row) & (lane8 == lane), full_sum(value), 0.0)
        loss_sum = jnp.sum(example[...], axis=0, keepdims=True)
        tile = tile + jnp.where((row8 == 0) & (lane8 == 4), loss_sum, 0.0)
        stat_send[step] = tile
        start(STATS)
        arrive(STATS)
        for k in range(1, n):
            tile = tile + stat_recv[step, k]
        losses[step] = jnp.broadcast_to(tile[0:1, 4:5] / batch_total, (8, LANES))

        row_id = lax.broadcasted_iota(jnp.int32, (8, 1), 0)
        share_of = jnp.where(row_id == 0, 1.0 / (rows1 * n * width_hidden), 1.0 / (rows2 * n * class_count))
        means = tile * share_of
        a, b, c, e = (means[:, i : i + 1] for i in range(4))
        step_share = (step.astype(F32) + 1.0) / steps
        z = [
            jnp.log(FLOOR + a),
            jnp.log(FLOOR + b),
            jnp.log(1.0 + c),
            e / jnp.sqrt((FLOOR + a) * (FLOOR + b)),
            jnp.full((8, 1), step_share, F32),
            jnp.ones((8, 1), F32),
            jnp.where(row_id == 0, 1.0, 0.0),
            jnp.where(row_id == 1, 1.0, 0.0),
        ]
        own_in = jnp.zeros((hin_ref.shape[0], hyper_rows), F32)
        for i in range(n):
            part = hin_ref[:, i * hyper_rows : (i + 1) * hyper_rows]
            own_in = own_in + jnp.where(me == i, part, 0.0)
        mixed = jnp.zeros((8, hyper_rows), F32)
        for i in range(hin_ref.shape[0]):
            mixed = mixed + z[i] * own_in[i : i + 1, :]
        opening = jnp.tanh(mixed)
        theta = mid_ref[...] + SIGMA * sign_ref[...] * noise_ref[...]
        part = jnp.dot(opening, theta, precision=HIGH, preferred_element_type=F32)
        share_send[step] = part
        start(SHARE)
        arrive(SHARE)
        for k in range(1, n):
            part = part + share_recv[step, k]
        middle = jnp.tanh(part)
        gen = jnp.dot(middle, hout[...], precision=HIGH, preferred_element_type=F32)

        neurons = (hout_ref.shape[1] - 1) // 5

        def update(tensor, gradient, moment, row, limit):
            def number(j):
                return gen[row : row + 1, j : j + 1]

            def spread(value):
                return jnp.broadcast_to(value, (8, LANES))

            by_grad = lax.rsqrt(FLOOR + a[row : row + 1])
            by_moment = lax.rsqrt(FLOOR + b[row : row + 1])
            rate = LR_BASE * jnp.exp(number(5 * neurons))
            coeffs = []
            for j in range(neurons):
                coeffs.append(
                    (
                        spread(number(3 * j) * by_grad),
                        spread(number(3 * j + 1) * by_moment),
                        spread(number(3 * j + 2)),
                        spread(number(3 * neurons + j)),
                        spread(number(4 * neurons + j)),
                    )
                )
            rate = spread(rate)

            @pl.loop(0, tensor.shape[0] // 8)
            def _(i):
                at = pl.ds(pl.multiple_of(i * 8, 8), 8)
                for column in range(0, tensor.shape[1], LANES):
                    cols = slice(column, column + LANES)
                    grad = gradient[at, cols]
                    mom = moment[at, cols]
                    value = tensor[at, cols]
                    direction = jnp.zeros_like(value)
                    for by_g, by_m, by_p, bias, gain in coeffs:
                        inner = by_g * grad + by_m * mom + by_p * value + bias
                        direction = direction + gain * jnp.maximum(inner, 0.0)
                    value = value - rate * direction
                    if column + LANES > limit:
                        value = jnp.where(lane8 + column < limit, value, 0.0)
                    tensor[at, cols] = value

        update(p1, g1, q1, 0, width_hidden)
        update(p2, g2, q2, 1, class_count)

        for stage in range(6):

            @pl.loop(1, n)
            def _(k):
                copy(stage, k).wait_send()

        return carry

    @pl.loop(1, tasks)
    def _(k):
        noise_copy(k).start()

    lax.fori_loop(0, steps, one_step, 0)

    score = jnp.zeros((8, LANES), F32)
    row = jnp.zeros((8, LANES), F32)
    for s in range(steps):
        score = score + losses[s]
        row = row + jnp.where(lane8 == s, losses[s], 0.0)
    score = score / steps
    loss_ref[...] = row[0:1, 0:steps]
    sign = sign_ref[...]
    score_send[...] = jnp.where(row8 < 4, score, sign)

    @pl.loop(1, tasks)
    def _(k):
        score_copy(k).start()

    new_out[...] = p2[:, 0:class_count]
    new_mom_out[...] = q2[:, 0:class_count]

    @pl.loop(1, tasks)
    def _(k):
        score_copy(k).wait_recv()
        noise_copy(k).wait_recv()

    center = score[0:1, 0:1]
    for k in range(1, tasks):
        center = center + score_recv[k][0:1, 0:1]
    center = center / tasks
    meta = sign * (score[0:1, 0:1] - center) * noise_ref[...]
    for k in range(1, tasks):
        other = score_recv[k]
        meta = meta + other[4:5, 0:1] * (other[0:1, 0:1] - center) * noise_recv[k]
    meta_ref[...] = meta / (SIGMA * tasks)

    @pl.loop(1, tasks)
    def _(k):
        score_copy(k).wait_send()
        noise_copy(k).wait_send()


def on_device(
    inputs,
    labels,
    w_hidden,
    w_out,
    mom_hidden,
    mom_out,
    signs,
    perturb,
    hyper_in,
    hyper_mid,
    hyper_out,
):
    n = lax.axis_size("dp")
    tasks = lax.axis_size("task")
    steps, local_batch, width_in = inputs.shape[1:]
    rows1, width_hidden = w_hidden.shape[1:]
    rows2, class_count = w_out.shape[1:]
    hyper_rows, hyper = hyper_mid.shape
    padded = -(-class_count // LANES) * LANES
    gens = -(-hyper_out.shape[1] // LANES) * LANES
    vmem = pl.BlockSpec(memory_space=pltpu.VMEM)
    out_shape = (
        jax.ShapeDtypeStruct((rows1, width_hidden), F32),
        jax.ShapeDtypeStruct((rows2, class_count), F32),
        jax.ShapeDtypeStruct((rows1, width_hidden), F32),
        jax.ShapeDtypeStruct((rows2, class_count), F32),
        jax.ShapeDtypeStruct((1, steps), F32),
        jax.ShapeDtypeStruct((hyper_rows, hyper), F32),
    )
    scratch = [
        pltpu.VMEM((steps, rows1 * n, width_hidden), BF16),
        pltpu.VMEM((steps, rows2 * n, padded), BF16),
        pltpu.VMEM((steps, rows1 * n, width_hidden), BF16),
        pltpu.VMEM((steps, rows2 * n, padded), BF16),
        pltpu.VMEM((steps, n, rows1, width_hidden), BF16),
        pltpu.VMEM((steps, n, rows2, padded), BF16),
        pltpu.VMEM((local_batch, width_hidden), BF16),
        pltpu.VMEM((local_batch, padded), BF16),
        pltpu.VMEM((local_batch, width_hidden), BF16),
        pltpu.VMEM((rows2, padded), F32),
        pltpu.VMEM((rows2, padded), F32),
        pltpu.VMEM((rows1, width_hidden), F32),
        pltpu.VMEM((rows2, padded), F32),
        pltpu.VMEM((local_batch, 1), F32),
        pltpu.VMEM((steps, 8, LANES), F32),
        pltpu.VMEM((steps, n, 8, LANES), F32),
        pltpu.VMEM((steps, 8, hyper), F32),
        pltpu.VMEM((steps, n, 8, hyper), F32),
        pltpu.VMEM((hyper, gens), F32),
        pltpu.VMEM((steps, 8, LANES), F32),
        pltpu.VMEM((hyper_rows, hyper), F32),
        pltpu.VMEM((tasks, hyper_rows, hyper), F32),
        pltpu.VMEM((8, LANES), F32),
        pltpu.VMEM((tasks, 8, LANES), F32),
        pltpu.SemaphoreType.DMA((steps, 6, n)),
        pltpu.SemaphoreType.DMA((steps, 6, n)),
        pltpu.SemaphoreType.DMA((2, tasks)),
        pltpu.SemaphoreType.DMA((2, tasks)),
    ]
    outs = pl.pallas_call(
        functools.partial(kernel, n, tasks),
        out_shape=out_shape,
        in_specs=[vmem] * 11,
        out_specs=(vmem,) * 6,
        scratch_shapes=scratch,
        compiler_params=pltpu.CompilerParams(
            collective_id=0, has_side_effects=True, vmem_limit_bytes=60 * 1024 * 1024
        ),
    )(
        inputs[0],
        labels[0][:, :, None],
        w_hidden[0],
        w_out[0],
        mom_hidden[0],
        mom_out[0],
        signs.astype(F32)[:, None],
        perturb[0],
        hyper_in,
        hyper_mid,
        hyper_out,
    )
    return tuple(out[None] for out in outs[:4]) + (outs[4], outs[5])


def solution(mesh):
    in_specs = (
        P("task", None, "dp", None),
        P("task", None, "dp"),
        P("task", "dp", None),
        P("task", "dp", None),
        P("task", "dp", None),
        P("task", "dp", None),
        P("task"),
        P("task", "dp", None),
        P(),
        P("dp", None),
        P(),
    )
    out_specs = (
        P("task", "dp", None),
        P("task", "dp", None),
        P("task", "dp", None),
        P("task", "dp", None),
        P("task", None),
        P("dp", None),
    )
    return jax.shard_map(
        on_device, mesh=mesh, in_specs=in_specs, out_specs=out_specs, check_vma=False
    )
```

```python
import functools

import jax
import jax.numpy as jnp
from jax import lax
from jax.experimental import pallas as pl
from jax.experimental.pallas import tpu as pltpu
from jax.sharding import PartitionSpec as P

BETA = 0.8
FLOOR = 0.001
SIGMA = 0.01
LR_BASE = 0.03
LANES = 128
HIGH = lax.Precision.HIGHEST
BY_ROWS = (((0,), (0,)), ((), ()))
BY_COLUMNS = (((1,), (1,)), ((), ()))
MESH = pl.DeviceIdType.MESH
F32 = jnp.float32
BF16 = jnp.bfloat16

HIDDEN_W, OUT_W, OUT_G, HIDDEN_G, STATS, SHARE = range(6)
NOISE, SCORE = range(2)


def fold(value):
    rows, columns = value.shape
    total = value[0:8]
    for row in range(8, rows, 8):
        total = total + value[row : row + 8]
    out = total[:, 0:LANES]
    for column in range(LANES, columns, LANES):
        out = out + total[:, column : column + LANES]
    return out


def full_sum(value):
    return jnp.sum(jnp.sum(value, axis=1, keepdims=True), axis=0, keepdims=True)


def kernel(
    n,
    tasks,
    x_ref,
    label_ref,
    w1_ref,
    w2_ref,
    m1_ref,
    m2_ref,
    sign_ref,
    noise_ref,
    hin_ref,
    mid_ref,
    hout_ref,
    p1,
    new_out,
    q1,
    new_mom_out,
    loss_ref,
    meta_ref,
    full1,
    full2,
    send1,
    send2,
    recv1,
    recv2,
    act,
    err,
    dpre,
    p2,
    q2,
    g1,
    g2,
    example,
    stat_send,
    stat_recv,
    share_send,
    share_recv,
    hout,
    losses,
    noise_send,
    noise_recv,
    score_send,
    score_recv,
    send_sem,
    recv_sem,
    task_send_sem,
    task_recv_sem,
):
    me = lax.axis_index("dp")
    task = lax.axis_index("task")
    line = n // 2
    place, side = me // 2, lax.rem(me, 2)
    partner = place * 2 + 1 - side
    steps, local_batch, width_in = x_ref.shape
    rows1 = w1_ref.shape[0]
    rows2, class_count = w2_ref.shape
    width_hidden = w1_ref.shape[1]
    padded = p2.shape[1]
    hyper_rows = mid_ref.shape[0]
    chunk = min(256, local_batch)
    block = min(256, width_hidden, width_in)
    scale_in = width_in ** (-0.5)
    scale_hidden = width_hidden ** (-0.5)
    batch_total = local_batch * n
    lane8 = lax.broadcasted_iota(jnp.int32, (8, LANES), 1)
    row8 = lax.broadcasted_iota(jnp.int32, (8, LANES), 0)

    barrier = pltpu.get_barrier_semaphore()

    @pl.loop(1, n)
    def _(k):
        pl.semaphore_signal(
            barrier, inc=1, device_id={"dp": lax.rem(me + k, n)}, device_id_type=MESH
        )

    @pl.loop(1, tasks)
    def _(k):
        pl.semaphore_signal(
            barrier, inc=1, device_id={"task": lax.rem(task + k, tasks)}, device_id_type=MESH
        )

    p1[...] = w1_ref[...]
    q1[...] = m1_ref[...]
    p2[...] = jnp.zeros_like(p2)
    q2[...] = jnp.zeros_like(q2)
    p2[:, 0:class_count] = w2_ref[...]
    q2[:, 0:class_count] = m2_ref[...]
    hout[...] = jnp.zeros_like(hout)
    hout[:, 0 : hout_ref.shape[1]] = hout_ref[...]
    noise_send[...] = noise_ref[...]
    pl.semaphore_wait(barrier, n - 1 + tasks - 1)

    def noise_copy(k):
        return pltpu.make_async_remote_copy(
            src_ref=noise_send,
            dst_ref=noise_recv.at[k],
            send_sem=task_send_sem.at[NOISE, k],
            recv_sem=task_recv_sem.at[NOISE, k],
            device_id={"task": lax.rem(task + k, tasks)},
            device_id_type=MESH,
        )

    def score_copy(k):
        return pltpu.make_async_remote_copy(
            src_ref=score_send,
            dst_ref=score_recv.at[k],
            send_sem=task_send_sem.at[SCORE, k],
            recv_sem=task_recv_sem.at[SCORE, k],
            device_id={"task": lax.rem(task + k, tasks)},
            device_id_type=MESH,
        )

    def one_step(step, carry):
        def small_copy(stage, k):
            if stage == STATS:
                source, target = stat_send.at[step], stat_recv.at[step, k]
            else:
                source, target = share_send.at[step], share_recv.at[step, k]
            return remote(stage, k, source, target, lax.rem(me + k, n))

        def remote(stage, k, source, target, peer):
            return pltpu.make_async_remote_copy(
                src_ref=source,
                dst_ref=target,
                send_sem=send_sem.at[step, stage, k],
                recv_sem=recv_sem.at[step, stage, k],
                device_id={"dp": peer},
                device_id_type=MESH,
            )

        def block_of(ref, owner, rows):
            return ref.at[step, pl.ds(pl.multiple_of(owner * rows, rows), rows)]

        def line_weight(stage, j):
            full, rows = (full1, rows1) if stage == HIDDEN_W else (full2, rows2)
            own = block_of(full, me, rows)
            return remote(stage, j, own, own, lax.rem(place + j, line) * 2 + side)

        def partner_weight(stage, j):
            full, rows = (full1, rows1) if stage == HIDDEN_W else (full2, rows2)
            held = block_of(full, lax.rem(place - j + line, line) * 2 + side, rows)
            return remote(stage, line + j, held, held, partner)

        def partner_grad(stage, j):
            sent, received, rows = (send2, recv2, rows2) if stage == OUT_G else (send1, recv1, rows1)
            owner = lax.rem(place + j, line) * 2 + 1 - side
            return remote(stage, line + j, block_of(sent, owner, rows), received.at[step, line + j], partner)

        def line_grad(stage, j):
            sent, received, rows = (send2, recv2, rows2) if stage == OUT_G else (send1, recv1, rows1)
            owner = lax.rem(place + j, line) * 2 + side
            return remote(stage, j, block_of(sent, owner, rows), received.at[step, j], owner)

        def start_weight(stage):
            partner_weight(stage, 0).start()

            @pl.loop(1, line)
            def _(j):
                line_weight(stage, j).start()

        def forward_weight(stage):
            @pl.loop(1, line)
            def _(j):
                line_weight(stage, j).wait_recv()
                partner_weight(stage, j).start()

        def arrive_weight(stage):
            @pl.loop(0, line)
            def _(j):
                partner_weight(stage, j).wait_recv()

        def start_grad(stage):
            @pl.loop(1, line)
            def _(j):
                partner_grad(stage, j).start()

            partner_grad(stage, 0).start()

        def forward_grad(stage):
            sent, received, rows = (send2, recv2, rows2) if stage == OUT_G else (send1, recv1, rows1)

            @pl.loop(1, line)
            def _(j):
                partner_grad(stage, j).wait_recv()
                base = pl.multiple_of((lax.rem(place + j, line) * 2 + side) * rows, rows)

                @pl.loop(0, rows // 16)
                def _(i):
                    at = pl.ds(pl.multiple_of(base + i * 16, 16), 16)
                    other = received[step, line + j, pl.ds(pl.multiple_of(i * 16, 16), 16), :]
                    both = sent[step, at, :].astype(F32) + other.astype(F32)
                    sent[step, at, :] = both.astype(BF16)

                line_grad(stage, j).start()

        def arrive_grad(stage):
            partner_grad(stage, 0).wait_recv()

            @pl.loop(1, line)
            def _(j):
                line_grad(stage, j).wait_recv()

        def start(stage):
            @pl.loop(1, n)
            def _(k):
                small_copy(stage, k).start()

        def arrive(stage):
            @pl.loop(1, n)
            def _(k):
                small_copy(stage, k).wait_recv()

        full1[step, pl.ds(pl.multiple_of(me * rows1, rows1), rows1)] = p1[...].astype(BF16)
        full2[step, pl.ds(pl.multiple_of(me * rows2, rows2), rows2)] = p2[...].astype(BF16)
        start_weight(HIDDEN_W)
        start_weight(OUT_W)
        forward_weight(HIDDEN_W)
        arrive_weight(HIDDEN_W)

        @pl.loop(0, local_batch // chunk)
        def _(i):
            at = pl.ds(pl.multiple_of(i * chunk, chunk), chunk)
            pre = jnp.dot(x_ref[step, at, :], full1[step], preferred_element_type=F32)
            act[at, :] = jnp.maximum(pre * scale_in, 0.0).astype(BF16)

        forward_weight(OUT_W)
        arrive_weight(OUT_W)

        @pl.loop(0, local_batch // chunk)
        def _(i):
            at = pl.ds(pl.multiple_of(i * chunk, chunk), chunk)
            logits = jnp.dot(act[at, :], full2[step], preferred_element_type=F32) * scale_hidden
            column = lax.broadcasted_iota(jnp.int32, logits.shape, 1)
            logits = jnp.where(column < class_count, logits, -jnp.inf)
            shifted = logits - jnp.max(logits, axis=1, keepdims=True)
            weight = jnp.exp(shifted)
            total = jnp.sum(weight, axis=1, keepdims=True)
            hit = column == label_ref[step, at, :]
            picked = jnp.sum(jnp.where(hit, shifted, 0.0), axis=1, keepdims=True)
            example[at, :] = jnp.log(total) - picked
            err[at, :] = (weight * (1.0 / total) - jnp.where(hit, 1.0, 0.0)).astype(BF16)

        @pl.loop(0, width_hidden // block)
        def _(i):
            at = pl.ds(pl.multiple_of(i * block, block), block)
            grad = lax.dot_general(act[:, at], err[...], BY_ROWS, preferred_element_type=F32)
            send2[step, at, :] = grad.astype(BF16)

        start_grad(OUT_G)

        @pl.loop(0, local_batch // chunk)
        def _(i):
            at = pl.ds(pl.multiple_of(i * chunk, chunk), chunk)
            back = lax.dot_general(err[at, :], full2[step], BY_COLUMNS, preferred_element_type=F32)
            live = act[at, :].astype(F32) > 0.0
            dpre[at, :] = jnp.where(live, back * scale_hidden, 0.0).astype(BF16)

        @pl.loop(0, width_in // block)
        def _(i):
            at = pl.ds(pl.multiple_of(i * block, block), block)
            grad = lax.dot_general(x_ref[step, :, at], dpre[...], BY_ROWS, preferred_element_type=F32)
            send1[step, at, :] = grad.astype(BF16)

        start_grad(HIDDEN_G)
        forward_grad(OUT_G)
        forward_grad(HIDDEN_G)

        def reduce(sent, received, gradient, moment, tensor, rows, scale):
            def body(i, sums):
                offset = pl.multiple_of(i * 16, 16)
                at = pl.ds(offset, 16)
                own = pl.ds(pl.multiple_of(me * rows + offset, 16), 16)
                grad = sent[step, own, :].astype(F32)
                for k in range(1, line + 1):
                    grad = grad + received[step, k, at, :].astype(F32)
                grad = grad * scale
                mom = BETA * moment[at, :] + (1.0 - BETA) * grad
                value = tensor[at, :]
                gradient[at, :] = grad
                moment[at, :] = mom
                return (
                    sums[0] + fold(grad * grad),
                    sums[1] + fold(mom * mom),
                    sums[2] + fold(value * value),
                    sums[3] + fold(grad * mom),
                )

            zero = jnp.zeros((8, LANES), F32)
            return lax.fori_loop(0, rows // 16, body, (zero, zero, zero, zero))

        arrive_grad(OUT_G)
        sums2 = reduce(send2, recv2, g2, q2, p2, rows2, scale_hidden)
        arrive_grad(HIDDEN_G)
        sums1 = reduce(send1, recv1, g1, q1, p1, rows1, scale_in)
        tile = jnp.zeros((8, LANES), F32)
        for row, sums in enumerate((sums1, sums2)):
            for lane, value in enumerate(sums):
                tile = tile + jnp.where((row8 == row) & (lane8 == lane), full_sum(value), 0.0)
        loss_sum = jnp.sum(example[...], axis=0, keepdims=True)
        tile = tile + jnp.where((row8 == 0) & (lane8 == 4), loss_sum, 0.0)
        stat_send[step] = tile
        start(STATS)
        arrive(STATS)
        for k in range(1, n):
            tile = tile + stat_recv[step, k]
        losses[step] = jnp.broadcast_to(tile[0:1, 4:5] / batch_total, (8, LANES))

        row_id = lax.broadcasted_iota(jnp.int32, (8, 1), 0)
        share_of = jnp.where(row_id == 0, 1.0 / (rows1 * n * width_hidden), 1.0 / (rows2 * n * class_count))
        means = tile * share_of
        a, b, c, e = (means[:, i : i + 1] for i in range(4))
        step_share = (step.astype(F32) + 1.0) / steps
        z = [
            jnp.log(FLOOR + a),
            jnp.log(FLOOR + b),
            jnp.log(1.0 + c),
            e / jnp.sqrt((FLOOR + a) * (FLOOR + b)),
            jnp.full((8, 1), step_share, F32),
            jnp.ones((8, 1), F32),
            jnp.where(row_id == 0, 1.0, 0.0),
            jnp.where(row_id == 1, 1.0, 0.0),
        ]
        own_in = jnp.zeros((hin_ref.shape[0], hyper_rows), F32)
        for i in range(n):
            part = hin_ref[:, i * hyper_rows : (i + 1) * hyper_rows]
            own_in = own_in + jnp.where(me == i, part, 0.0)
        mixed = jnp.zeros((8, hyper_rows), F32)
        for i in range(hin_ref.shape[0]):
            mixed = mixed + z[i] * own_in[i : i + 1, :]
        opening = jnp.tanh(mixed)
        theta = mid_ref[...] + SIGMA * sign_ref[...] * noise_ref[...]
        part = jnp.dot(opening, theta, precision=HIGH, preferred_element_type=F32)
        share_send[step] = part
        start(SHARE)
        arrive(SHARE)
        for k in range(1, n):
            part = part + share_recv[step, k]
        middle = jnp.tanh(part)
        gen = jnp.dot(middle, hout[...], precision=HIGH, preferred_element_type=F32)

        neurons = (hout_ref.shape[1] - 1) // 5

        def update(tensor, gradient, moment, row, limit):
            def number(j):
                return gen[row : row + 1, j : j + 1]

            def spread(value):
                return jnp.broadcast_to(value, (8, LANES))

            by_grad = lax.rsqrt(FLOOR + a[row : row + 1])
            by_moment = lax.rsqrt(FLOOR + b[row : row + 1])
            rate = LR_BASE * jnp.exp(number(5 * neurons))
            coeffs = []
            for j in range(neurons):
                coeffs.append(
                    (
                        spread(number(3 * j) * by_grad),
                        spread(number(3 * j + 1) * by_moment),
                        spread(number(3 * j + 2)),
                        spread(number(3 * neurons + j)),
                        spread(number(4 * neurons + j)),
                    )
                )
            rate = spread(rate)

            @pl.loop(0, tensor.shape[0] // 8)
            def _(i):
                at = pl.ds(pl.multiple_of(i * 8, 8), 8)
                for column in range(0, tensor.shape[1], LANES):
                    cols = slice(column, column + LANES)
                    grad = gradient[at, cols]
                    mom = moment[at, cols]
                    value = tensor[at, cols]
                    direction = jnp.zeros_like(value)
                    for by_g, by_m, by_p, bias, gain in coeffs:
                        inner = by_g * grad + by_m * mom + by_p * value + bias
                        direction = direction + gain * jnp.maximum(inner, 0.0)
                    value = value - rate * direction
                    if column + LANES > limit:
                        value = jnp.where(lane8 + column < limit, value, 0.0)
                    tensor[at, cols] = value

        update(p1, g1, q1, 0, width_hidden)
        update(p2, g2, q2, 1, class_count)

        for stage in (HIDDEN_W, OUT_W):

            @pl.loop(0, line)
            def _(j):
                partner_weight(stage, j).wait_send()

            @pl.loop(1, line)
            def _(j):
                line_weight(stage, j).wait_send()

        for stage in (OUT_G, HIDDEN_G):

            @pl.loop(0, line)
            def _(j):
                partner_grad(stage, j).wait_send()

            @pl.loop(1, line)
            def _(j):
                line_grad(stage, j).wait_send()

        for stage in (STATS, SHARE):

            @pl.loop(1, n)
            def _(k):
                small_copy(stage, k).wait_send()

        return carry

    @pl.loop(1, tasks)
    def _(k):
        noise_copy(k).start()

    lax.fori_loop(0, steps, one_step, 0)

    score = jnp.zeros((8, LANES), F32)
    row = jnp.zeros((8, LANES), F32)
    for s in range(steps):
        score = score + losses[s]
        row = row + jnp.where(lane8 == s, losses[s], 0.0)
    score = score / steps
    loss_ref[...] = row[0:1, 0:steps]
    sign = sign_ref[...]
    score_send[...] = jnp.where(row8 < 4, score, sign)

    @pl.loop(1, tasks)
    def _(k):
        score_copy(k).start()

    new_out[...] = p2[:, 0:class_count]
    new_mom_out[...] = q2[:, 0:class_count]

    @pl.loop(1, tasks)
    def _(k):
        score_copy(k).wait_recv()
        noise_copy(k).wait_recv()

    center = score[0:1, 0:1]
    for k in range(1, tasks):
        center = center + score_recv[k][0:1, 0:1]
    center = center / tasks
    meta = sign * (score[0:1, 0:1] - center) * noise_ref[...]
    for k in range(1, tasks):
        other = score_recv[k]
        meta = meta + other[4:5, 0:1] * (other[0:1, 0:1] - center) * noise_recv[k]
    meta_ref[...] = meta / (SIGMA * tasks)

    @pl.loop(1, tasks)
    def _(k):
        score_copy(k).wait_send()
        noise_copy(k).wait_send()


def on_device(
    inputs,
    labels,
    w_hidden,
    w_out,
    mom_hidden,
    mom_out,
    signs,
    perturb,
    hyper_in,
    hyper_mid,
    hyper_out,
):
    n = lax.axis_size("dp")
    tasks = lax.axis_size("task")
    steps, local_batch, width_in = inputs.shape[1:]
    rows1, width_hidden = w_hidden.shape[1:]
    rows2, class_count = w_out.shape[1:]
    hyper_rows, hyper = hyper_mid.shape
    padded = -(-class_count // LANES) * LANES
    gens = -(-hyper_out.shape[1] // LANES) * LANES
    vmem = pl.BlockSpec(memory_space=pltpu.VMEM)
    out_shape = (
        jax.ShapeDtypeStruct((rows1, width_hidden), F32),
        jax.ShapeDtypeStruct((rows2, class_count), F32),
        jax.ShapeDtypeStruct((rows1, width_hidden), F32),
        jax.ShapeDtypeStruct((rows2, class_count), F32),
        jax.ShapeDtypeStruct((1, steps), F32),
        jax.ShapeDtypeStruct((hyper_rows, hyper), F32),
    )
    scratch = [
        pltpu.VMEM((steps, rows1 * n, width_hidden), BF16),
        pltpu.VMEM((steps, rows2 * n, padded), BF16),
        pltpu.VMEM((steps, rows1 * n, width_hidden), BF16),
        pltpu.VMEM((steps, rows2 * n, padded), BF16),
        pltpu.VMEM((steps, n, rows1, width_hidden), BF16),
        pltpu.VMEM((steps, n, rows2, padded), BF16),
        pltpu.VMEM((local_batch, width_hidden), BF16),
        pltpu.VMEM((local_batch, padded), BF16),
        pltpu.VMEM((local_batch, width_hidden), BF16),
        pltpu.VMEM((rows2, padded), F32),
        pltpu.VMEM((rows2, padded), F32),
        pltpu.VMEM((rows1, width_hidden), F32),
        pltpu.VMEM((rows2, padded), F32),
        pltpu.VMEM((local_batch, 1), F32),
        pltpu.VMEM((steps, 8, LANES), F32),
        pltpu.VMEM((steps, n, 8, LANES), F32),
        pltpu.VMEM((steps, 8, hyper), F32),
        pltpu.VMEM((steps, n, 8, hyper), F32),
        pltpu.VMEM((hyper, gens), F32),
        pltpu.VMEM((steps, 8, LANES), F32),
        pltpu.VMEM((hyper_rows, hyper), F32),
        pltpu.VMEM((tasks, hyper_rows, hyper), F32),
        pltpu.VMEM((8, LANES), F32),
        pltpu.VMEM((tasks, 8, LANES), F32),
        pltpu.SemaphoreType.DMA((steps, 6, n)),
        pltpu.SemaphoreType.DMA((steps, 6, n)),
        pltpu.SemaphoreType.DMA((2, tasks)),
        pltpu.SemaphoreType.DMA((2, tasks)),
    ]
    outs = pl.pallas_call(
        functools.partial(kernel, n, tasks),
        out_shape=out_shape,
        in_specs=[vmem] * 11,
        out_specs=(vmem,) * 6,
        scratch_shapes=scratch,
        compiler_params=pltpu.CompilerParams(
            collective_id=0, has_side_effects=True, vmem_limit_bytes=60 * 1024 * 1024
        ),
    )(
        inputs[0],
        labels[0][:, :, None],
        w_hidden[0],
        w_out[0],
        mom_hidden[0],
        mom_out[0],
        signs.astype(F32)[:, None],
        perturb[0],
        hyper_in,
        hyper_mid,
        hyper_out,
    )
    return tuple(out[None] for out in outs[:4]) + (outs[4], outs[5])


def solution(mesh):
    in_specs = (
        P("task", None, "dp", None),
        P("task", None, "dp"),
        P("task", "dp", None),
        P("task", "dp", None),
        P("task", "dp", None),
        P("task", "dp", None),
        P("task"),
        P("task", "dp", None),
        P(),
        P("dp", None),
        P(),
    )
    out_specs = (
        P("task", "dp", None),
        P("task", "dp", None),
        P("task", "dp", None),
        P("task", "dp", None),
        P("task", None),
        P("dp", None),
    )
    return jax.shard_map(
        on_device, mesh=mesh, in_specs=in_specs, out_specs=out_specs, check_vma=False
    )
```
